32 devices in a mesh: groups: 2 (over x), lon: 8 (over z, y), lat: 2 (over core).
Axes of the slice: x: 2, y: 2, z: 4, core: 2. Of those that a mesh axis runs over, the one named last changes fastest.
Arguments:
- fields: bfloat16 [24, 1024, 128], P(('groups', 'lat'), 'lon'), parts along dimension 0, may hold values from -6 to 6
- norm_gain: float32 [128], replicated, may hold values from 0.5 to 1.5
- w_qkv: bfloat16 [128, 384], replicated, may hold values from -5.303301 to 5.303301
- w_out: bfloat16 [128, 128], replicated, may hold values from -0.5 to 0.5
Outputs:
- updated: bfloat16 [24, 1024, 128], P(('groups', 'lat'), 'lon'), parts along dimension 0
The draws below stay inside these ranges and needn't reach their ends.
There are 2 independent parts, one for each index of `groups`. The reference program is written for one: setup_inputs(seed, part) draws one part's arguments, and reference() takes and returns one part's arrays. A program takes and returns all parts, laid end to end along the dimension named above; an argument that names none is the same for every part. Nothing has to cross between parts.
All inputs are finite; a program needn't handle non-finite values.
Results may differ from the reference program's by a relative error of at most 0.005.
The reference program's roundings to bfloat16 on the way (of `normed`, `weights` and `attended`) count: a program that leaves them out, or rounds other values in their place, can miss the bound.
Values may be sent and summed in bfloat16 or wider, within the bound.
A program may use at most 128 MiB of HBM per device.

```python
import math
import jax
import jax.numpy as jnp
from jax import lax

HEADS = 8
HEAD_DIM = 16
C = 128
NLON = 1024
NLAT = 12


def draw_w_qkv(key, part):
    base = jnp.clip(jax.random.normal(key, (C, 3 * C), jnp.float32), -6.0, 6.0) * (2.0 / math.sqrt(C))
    return base.astype(jnp.bfloat16)


def block_scale(stream_key, shape, shards, low, high):
    def one(position, shards_of):
        steps = jax.random.uniform(jax.random.fold_in(jax.random.fold_in(stream_key, 6), position), (shards_of,), jnp.float32, low / len(shards), high / len(shards))
        return jnp.repeat(jnp.exp(steps), shape[position] // shards_of).reshape((-1,) + (1,) * (len(shape) - position - 1))

    loudness = one(*shards[0])
    for cut in shards[1:]:
        loudness = loudness * one(*cut)
    return loudness


def bell_draw(rng, dims, scale, bound, split=(), kind=jnp.bfloat16):
    values = scale * jax.random.normal(rng, dims, jnp.float32)
    if split:
        values = values * block_scale(rng, dims, split, -0.22, 0.18)
    return jnp.clip(values, -bound, bound).astype(kind)


def setup_inputs(seed: int = 0, part: int = 0) -> dict:
    key_list = jax.random.split(jax.random.key(seed), 5)
    part_keys = jax.random.split(jax.random.fold_in(key_list[4], part), 5)
    fields = bell_draw(part_keys[0], (NLAT, NLON, C), 1.0, 6.0, ((0, 2), (1, 8)))
    norm_gain = jnp.clip(1.0 + 0.1 * jax.random.normal(key_list[1], (C,), jnp.float32), 0.5, 1.5)
    w_qkv = draw_w_qkv(jax.random.fold_in(key_list[4], 71), part)
    w_out = bell_draw(key_list[3], (C, C), C ** -0.5, 0.5)
    return {"fields": fields, "norm_gain": norm_gain, "w_qkv": w_qkv, "w_out": w_out}


def reference(fields, norm_gain, w_qkv, w_out):
    width = HEADS * HEAD_DIM
    inputs = fields.astype(jnp.float32)
    center = lax.optimization_barrier(jnp.mean(inputs, axis=-1, keepdims=True))
    spread = lax.optimization_barrier(jnp.mean((inputs - center) ** 2, axis=-1, keepdims=True))
    normed = ((inputs - center) * lax.rsqrt(spread + 1e-05) * norm_gain).astype(jnp.bfloat16)
    projected = jnp.dot(normed.reshape(-1, width), w_qkv, preferred_element_type=jnp.float32)
    projected = projected.reshape(NLAT, NLON, 3 * width)
    queries = (projected[..., :width] * (1.0 / math.sqrt(HEAD_DIM))).astype(jnp.bfloat16)
    keys = projected[..., width:2 * width].astype(jnp.bfloat16)
    values = projected[..., 2 * width:].astype(jnp.bfloat16)
    block = math.gcd(NLON, 512)

    def one_row(operands):
        row_queries, row_keys, row_values = operands
        key_heads = row_keys.reshape(NLON, HEADS, HEAD_DIM).astype(jnp.float32)
        value_heads = row_values.reshape(NLON, HEADS, HEAD_DIM).astype(jnp.float32)
        query_blocks = row_queries.reshape(NLON // block, block, HEADS, HEAD_DIM)

        def one_block(query_block):
            scores = jnp.einsum('qhd,khd->hqk', query_block.astype(jnp.float32), key_heads)
            highest = lax.optimization_barrier(jnp.max(scores, axis=-1, keepdims=True))
            expd = jnp.exp(scores - highest)
            totals = lax.optimization_barrier(jnp.sum(expd, axis=-1))
            weights = expd.astype(jnp.bfloat16).astype(jnp.float32)
            mixed = jnp.einsum('hqk,khd->qhd', weights, value_heads)
            mixed = mixed / jnp.transpose(totals)[:, :, None]
            return mixed.reshape(block, width).astype(jnp.bfloat16)
        return lax.map(one_block, query_blocks).reshape(NLON, width)
    attended = lax.map(one_row, (queries, keys, values))
    output = jnp.dot(attended.reshape(-1, width), w_out, preferred_element_type=jnp.float32)
    return (inputs + output.reshape(NLAT, NLON, width)).astype(jnp.bfloat16)
```

```python
import functools
import math

import jax
import jax.numpy as jnp
from jax import lax
from jax.experimental import pallas as pl
from jax.experimental.pallas import tpu as pltpu
from jax.sharding import PartitionSpec as P

HEADS = 8
LOG2E = math.log2(math.e)
MESH = pl.DeviceIdType.MESH


def dot(a, b, contract):
    return lax.dot_general(a, b, ((contract[:1], contract[1:]), ((), ())), preferred_element_type=jnp.float32)


def kernel(n, per, slots, fields_hbm, gain_hbm, wqkv_hbm, wout_hbm, out_ref,
           fields_ref, gain_ref, wqkv_ref, wout_ref, loaded,
           normed, whole, w_t, scores_a, scores_b, scores_c, q_s, k_s, v_s,
           mixed, returned,
           send1, recv1, send2, recv2):
    me = lax.axis_index("lon")
    rows, cells, width = fields_ref.shape
    head_width = width // HEADS
    total = n * cells
    block = math.gcd(total, 512)
    chunk = math.gcd(total, 256)

    def partner(k):
        if n & (n - 1):
            return lax.rem(me + n - k, n)
        mate = 0
        for bit in range(n.bit_length() - 1):
            own = lax.rem(me // (1 << bit), 2)
            mate = mate + ((1 - own) if (k >> bit) & 1 else own) * (1 << bit)
        return mate

    barrier = pltpu.get_barrier_semaphore()
    for k in range(1, n):
        pl.semaphore_signal(barrier, inc=1, device_id={"lon": lax.rem(me + k, n)}, device_id_type=MESH)

    loads = [
        pltpu.make_async_copy(src, dst, loaded.at[i])
        for i, (src, dst) in enumerate((
            (fields_hbm, fields_ref), (gain_hbm, gain_ref), (wqkv_hbm, wqkv_ref), (wout_hbm, wout_ref),
        ))
    ]
    for load in loads:
        load.start()
    for load in loads:
        load.wait()

    gain = gain_ref[...]
    for r in range(rows):
        inputs = fields_ref[r].astype(jnp.float32)
        center = jnp.mean(inputs, axis=-1, keepdims=True)
        spread = jnp.mean((inputs - center) ** 2, axis=-1, keepdims=True)
        normed[r] = ((inputs - center) * lax.rsqrt(spread + 1e-05) * gain).astype(jnp.bfloat16)

    def first_row(d):
        return (d * per) // HEADS

    def last_row(d):
        return (d * per + per - 1) // HEADS

    pl.semaphore_wait(barrier, n - 1)

    def forward(j, k):
        d = partner(k)
        return d, pltpu.make_async_remote_copy(
            src_ref=normed.at[first_row(d) + j],
            dst_ref=whole.at[j, me],
            send_sem=send1.at[j, k],
            recv_sem=recv1.at[j, me],
            device_id={"lon": d},
            device_id_type=MESH,
        )

    for j in range(slots):
        for k in range(n - 1, 0, -1):
            d, copy = forward(j, k)

            @pl.when(first_row(d) + j <= last_row(d))
            def _():
                copy.start()

    for j in range(slots):
        @pl.when(first_row(me) + j <= last_row(me))
        def _():
            whole[j, me] = normed[first_row(me) + j]

    w_t[...] = wqkv_ref[...].astype(jnp.float32).T.astype(jnp.bfloat16)

    def back(t, k):
        d = partner(k)
        return pltpu.make_async_remote_copy(
            src_ref=mixed.at[t, d],
            dst_ref=returned.at[me * per + t],
            send_sem=send2.at[t, k],
            recv_sem=recv2.at[me * per + t],
            device_id={"lon": d},
            device_id_type=MESH,
        )

    def wait_slot(slot):
        for k in range(1, n):
            src = lax.rem(me + k, n)
            pltpu.make_async_remote_copy(
                src_ref=normed.at[0],
                dst_ref=whole.at[slot, src],
                send_sem=send1.at[0, 0],
                recv_sem=recv1.at[slot, src],
                device_id={"lon": src},
                device_id_type=MESH,
            ).wait_recv()

    def project(item):
        head = lax.rem(item, HEADS)
        cell_rows = whole[item // HEADS - first_row(me)].reshape(total, width)

        def weight(part):
            start = pl.multiple_of(part * width + head * head_width, head_width)
            return w_t[pl.ds(start, head_width), :]

        w_k = weight(1)
        q_t = (dot(weight(0), cell_rows, (1, 1)) * (1.0 / math.sqrt(head_width))).astype(jnp.bfloat16)
        q_t = q_t.astype(jnp.float32) * LOG2E
        q_hi = q_t.astype(jnp.bfloat16)
        q_lo = (q_t - q_hi.astype(jnp.float32)).astype(jnp.bfloat16)
        q_s[...] = jnp.concatenate([q_hi, q_lo], axis=0)
        k_s[...] = dot(cell_rows, jnp.concatenate([w_k, w_k], axis=0), (1, 1)).astype(jnp.bfloat16)
        v_s[...] = dot(weight(2), cell_rows, (1, 1)).astype(jnp.bfloat16)

    def buffer(b):
        return scores_c if b == 0 else (scores_a, scores_b)[b % 2]

    def first_pass(b, queries, keys):
        q_block = queries[:, b * block:(b + 1) * block]
        highest = None
        for c in range(total // chunk):
            s = dot(keys[c * chunk:(c + 1) * chunk], q_block, (1, 0))
            buffer(b)[pl.ds(c * chunk, chunk), :] = s
            part = jnp.max(s.reshape(chunk // 8, 8, block), axis=0)
            highest = part if highest is None else jnp.maximum(highest, part)
        return jnp.max(highest, axis=0, keepdims=True)

    def second_pass(b, highest, v_t):
        sums = jnp.zeros((8, block), jnp.float32)
        acc = jnp.zeros((head_width, block), jnp.float32)
        for c in range(total // chunk):
            p = jnp.exp2(buffer(b)[pl.ds(c * chunk, chunk), :] - highest)
            sums = sums + jnp.sum(p.reshape(chunk // 8, 8, block), axis=0)
            acc = acc + dot(v_t[:, c * chunk:(c + 1) * chunk], p.astype(jnp.bfloat16), (1, 0))
        return (acc / jnp.sum(sums, axis=0, keepdims=True)).astype(jnp.bfloat16)

    def one_item(t, highest):
        item = me * per + t
        after = jnp.minimum(item + 1, me * per + per - 1)

        @pl.when((t + 1 < per) & (lax.rem(item + 1, HEADS) == 0))
        def _():
            wait_slot(after // HEADS - first_row(me))

        queries, keys, v_t = q_s[...], k_s[...], v_s[...]
        project(after)
        blocks = total // block
        for b in range(blocks):
            if b + 1 < blocks:
                following = first_pass(b + 1, queries, keys)
            done = second_pass(b, highest, v_t)
            if b + 1 == blocks:
                following = first_pass(0, q_s[...], k_s[...])
            highest = following
            for s in range(block // cells):
                mixed[t, b * (block // cells) + s] = done[:, s * cells:(s + 1) * cells]

        returned[item] = mixed[t, me]
        for k in range(n - 1, 0, -1):
            back(t, k).start()
        return highest

    wait_slot(0)
    project(me * per)
    lax.fori_loop(0, per, one_item, first_pass(0, q_s[...], k_s[...]))

    def finish(t, carry):
        for k in range(1, n):
            src = lax.rem(me + k, n)
            pltpu.make_async_remote_copy(
                src_ref=mixed.at[0, 0],
                dst_ref=returned.at[src * per + t],
                send_sem=send2.at[t, k],
                recv_sem=recv2.at[src * per + t],
                device_id={"lon": src},
                device_id_type=MESH,
            ).wait_recv()
        return carry

    lax.fori_loop(0, per, finish, 0)

    for r in range(rows):
        att_t = returned[pl.ds(r * HEADS, HEADS)].reshape(width, cells)
        update = dot(att_t, wout_ref[...], (0, 0))
        out_ref[r] = (fields_ref[r].astype(jnp.float32) + update).astype(jnp.bfloat16)

    for j in range(slots):
        for k in range(1, n):
            d, copy = forward(j, k)

            @pl.when(first_row(d) + j <= last_row(d))
            def _():
                copy.wait_send()

    def sent(t, carry):
        for k in range(1, n):
            back(t, k).wait_send()
        return carry

    lax.fori_loop(0, per, sent, 0)


def solution(mesh):
    n = mesh.shape["lon"]

    def body(fields, norm_gain, w_qkv, w_out):
        rows, cells, width = fields.shape
        per = rows * HEADS // n
        slots = max((d * per + per - 1) // HEADS - (d * per) // HEADS + 1 for d in range(n))
        total = n * cells
        block = math.gcd(total, 512)
        return pl.pallas_call(
            functools.partial(kernel, n, per, slots),
            out_shape=pltpu.VMEM(fields.shape, fields.dtype),
            in_specs=[pl.BlockSpec(memory_space=pltpu.HBM)] * 4,
            out_specs=pl.BlockSpec(memory_space=pltpu.VMEM),
            scratch_shapes=[
                pltpu.VMEM(fields.shape, fields.dtype),
                pltpu.VMEM((1, width), norm_gain.dtype),
                pltpu.VMEM(w_qkv.shape, w_qkv.dtype),
                pltpu.VMEM(w_out.shape, w_out.dtype),
                pltpu.SemaphoreType.DMA((4,)),
                pltpu.VMEM((rows, cells, width), jnp.bfloat16),
                pltpu.VMEM((slots, n, cells, width), jnp.bfloat16),
                pltpu.VMEM((3 * width, width), jnp.bfloat16),
                pltpu.VMEM((total, block), jnp.float32),
                pltpu.VMEM((total, block), jnp.float32),
                pltpu.VMEM((total, block), jnp.float32),
                pltpu.VMEM((2 * width // HEADS, total), jnp.bfloat16),
                pltpu.VMEM((total, 2 * width // HEADS), jnp.bfloat16),
                pltpu.VMEM((width // HEADS, total), jnp.bfloat16),
                pltpu.VMEM((per, n, width // HEADS, cells), jnp.bfloat16),
                pltpu.VMEM((rows * HEADS, width // HEADS, cells), jnp.bfloat16),
                pltpu.SemaphoreType.DMA((slots, n)),
                pltpu.SemaphoreType.DMA((slots, n)),
                pltpu.SemaphoreType.DMA((per, n)),
                pltpu.SemaphoreType.DMA((rows * HEADS,)),
            ],
            compiler_params=pltpu.CompilerParams(
                collective_id=0, has_side_effects=True, vmem_limit_bytes=40 * 2**20,
            ),
        )(*(
            pltpu.with_memory_space_constraint(x, pltpu.HBM)
            for x in (fields, norm_gain.reshape(1, width), w_qkv, w_out)
        ))

    return jax.shard_map(
        body,
        mesh=mesh,
        in_specs=(P(("groups", "lat"), "lon", None), P(), P(), P()),
        out_specs=P(("groups", "lat"), "lon", None),
        check_vma=False,
    )
```

```python
import functools
import math

import jax
import jax.numpy as jnp
from jax import lax
from jax.experimental import pallas as pl
from jax.experimental.pallas import tpu as pltpu
from jax.sharding import PartitionSpec as P

HEADS = 8
LOG2E = math.log2(math.e)
MESH = pl.DeviceIdType.MESH


def dot(a, b, contract):
    return lax.dot_general(a, b, ((contract[:1], contract[1:]), ((), ())), preferred_element_type=jnp.float32)


def plan(n, m, rows):
    chips = max(c for c in range(m, n // 2 + 1, m) if n % c == 0 and (rows * m) % c == 0)
    rpc = rows * m // chips
    return chips, rpc, rpc // m


def kernel(n, m, fields_hbm, gain_hbm, wqkv_hbm, wout_hbm, out_ref,
           fields_ref, gain_ref, wqkv_ref, wout_ref,
           normed, w_t, x, scores_a, scores_b, q_s, kk_s, v_s, top_s, sum_s, acc_s, mixed, returned,
           loaded, send1, twin1, recv1, relayed, send2, recv2):
    me, lat = lax.axis_index("lon"), lax.axis_index("lat")
    rows, cells, width = fields_ref.shape
    head_width = width // HEADS
    chips, rpc, full = plan(n, m, rows)
    groups = n // chips
    share = HEADS // m
    half = share * head_width
    queries = chips * cells
    pair = 2
    block = pair * cells
    blocks = chips // pair
    per_lat = chips // m
    group, chip = me // chips, lax.rem(me, chips)
    source_lat = chip // per_lat
    first_row = lax.rem(chip, per_lat) * rpc
    mine = source_lat == lat
    other = 1 - lat
    shared = full if rpc % m else None
    slots = list(range(full)) + ([full] if rpc % m else [])

    barrier = pltpu.get_barrier_semaphore()
    for k in range(n):
        for c in range(m):
            if k or c:
                pl.semaphore_signal(
                    barrier, inc=1, device_id={"lon": lax.rem(me + k, n), "lat": lax.rem(lat + c, m)},
                    device_id_type=MESH)

    loads = [
        pltpu.make_async_copy(src, dst, loaded.at[i])
        for i, (src, dst) in enumerate((
            (fields_hbm, fields_ref), (gain_hbm, gain_ref), (wqkv_hbm, wqkv_ref), (wout_hbm, wout_ref),
        ))
    ]
    for load in loads:
        load.start()
    loads[1].wait()
    loads[0].wait()

    gain = gain_ref[...]
    for r in range(rows):
        inputs = fields_ref[r].astype(jnp.float32)
        center = jnp.mean(inputs, axis=-1, keepdims=True)
        spread = jnp.mean((inputs - center) ** 2, axis=-1, keepdims=True)
        normed[r] = ((inputs - center) * lax.rsqrt(spread + 1e-05) * gain).astype(jnp.bfloat16)

    def slot_row(slot):
        if slot == shared:
            return first_row + full
        return first_row + slot + lat * (rpc - full)

    def remote(src, dst, send, recv, lon, core):
        return pltpu.make_async_remote_copy(
            src_ref=src, dst_ref=dst, send_sem=send, recv_sem=recv,
            device_id={"lon": lon, "lat": core}, device_id_type=MESH)

    def forward(k, r):
        lon = lax.rem(group + k, groups) * chips + lat * per_lat + r // rpc
        w = r % rpc
        if w < full:
            slot, core = w, 0
        elif w >= rpc - full:
            slot, core = w - (rpc - full), 1
        else:
            slot, core = full, lax.rem(me, m)
        away = True if k else (lon != me)
        if not k and slot != shared:
            away = (lon != me) | (core != lat)
        copy = remote(normed.at[r], x.at[slot, me], send1.at[k, r], recv1.at[slot, me], lon, core)
        twin = None
        if not k and slot == shared:
            twin = remote(normed.at[r], x.at[slot, me], twin1.at[r], recv1.at[slot, me], me, other)
        return slot, away, copy, twin

    order = [r for r in range(rows) if full <= r % rpc < rpc - full] + [
        r for r in range(rows) if not full <= r % rpc < rpc - full]

    def each_forward(use):
        for k in range(groups):
            for r in order:
                slot, away, copy, twin = forward(k, r)
                if away is True:
                    use(copy)
                    continue

                @pl.when(away)
                def _():
                    use(copy)

                if twin is not None:
                    @pl.when(jnp.logical_not(away))
                    def _():
                        use(twin)

    pl.semaphore_wait(barrier, n * m - 1)
    each_forward(lambda copy: copy.start())

    @pl.when(mine)
    def _():
        for slot in slots:
            x[slot, me] = normed[slot_row(slot)]

    loads[2].wait()
    loads[3].wait()
    w_t[...] = wqkv_ref[...].astype(jnp.float32).T.astype(jnp.bfloat16)
    top_s[...] = jnp.full(top_s.shape, -jnp.inf, jnp.float32)
    sum_s[...] = jnp.zeros(sum_s.shape, jnp.float32)
    acc_s[...] = jnp.zeros(acc_s.shape, jnp.float32)

    def arrival(slot, s):
        return remote(normed.at[0], x.at[slot, s], send1.at[0, 0], recv1.at[slot, s], s, lat)

    def relay(s):
        return remote(x.at[full, s], x.at[full, s], relayed.at[s], recv1.at[full, s], me, other)

    def pass_on(k):
        if shared is None:
            return
        for c in range(chips):
            s = lax.rem(group + k, groups) * chips + c

            @pl.when((s != me) & (lax.rem(s, m) == lat))
            def _():
                arrival(full, s).wait_recv()
                relay(s).start()

    def weight(part, slot):
        start = part * width
        if slot != shared:
            return w_t[start:start + width, :]
        return w_t[pl.ds(pl.multiple_of(start + lat * half, half), half), :]

    def await_source(slot, s):
        if slot == shared:
            due = jnp.where(s == me, jnp.logical_not(mine), lax.rem(s, m) != lat)
        else:
            due = (s != me) | jnp.logical_not(mine)

        @pl.when(due)
        def _():
            arrival(slot, s).wait_recv()

    def heads_of(slot):
        return share if slot == shared else HEADS

    def project_queries(slot):
        span = heads_of(slot) * head_width
        for b in range(blocks):
            cell_rows = x[slot, pl.ds(group * chips + b * pair, pair)].reshape(block, width)
            q_t = (dot(weight(0, slot), cell_rows, (1, 1)) * (1.0 / math.sqrt(head_width))).astype(jnp.bfloat16)
            q_t = q_t.astype(jnp.float32) * LOG2E
            q_hi = q_t.astype(jnp.bfloat16)
            q_lo = (q_t - q_hi.astype(jnp.float32)).astype(jnp.bfloat16)
            q_s[slot, 0:span, b * block:(b + 1) * block] = q_hi
            q_s[slot, width:width + span, b * block:(b + 1) * block] = q_lo

    def attend(slot, s0):
        heads = heads_of(slot)
        span = heads * head_width
        cell_rows = x[slot, pl.ds(s0, pair)].reshape(block, width)
        w_k = weight(1, slot)
        if slot == shared:
            kk_s[:, 0:2 * span] = dot(cell_rows, jnp.concatenate([w_k, w_k], axis=0), (1, 1)).astype(jnp.bfloat16)
        else:
            keys = dot(cell_rows, w_k, (1, 1)).astype(jnp.bfloat16)
            kk_s[:, 0:span] = keys
            kk_s[:, span:2 * span] = keys
        v_s[0:span, :] = dot(weight(2, slot), cell_rows, (1, 1)).astype(jnp.bfloat16)

        def gap(size):
            return [jnp.zeros((size, queries), jnp.bfloat16)] if size else []

        def first_pass(h):
            lo, hi = h * head_width, (h + 1) * head_width
            spread_q = jnp.concatenate(
                gap(lo) + [q_s[slot, lo:hi, :]] + gap(span - hi + lo) + [q_s[slot, width + lo:width + hi, :]]
                + gap(span - hi), axis=0)
            s = dot(kk_s[:, 0:2 * span], spread_q, (1, 0))
            (scores_a, scores_b)[h % 2][...] = s
            return jnp.max(jnp.max(s.reshape(block // 8, 8, queries), axis=0), axis=0, keepdims=True)

        def second_pass(h, highest):
            at = slot * HEADS + h
            before = top_s[at]
            now = jnp.maximum(before, highest)
            fade = jnp.exp2(before - now)
            top_s[at] = now
            p = jnp.exp2((scores_a, scores_b)[h % 2][...] - now)
            sum_s[at] = sum_s[at] * fade + jnp.sum(p.reshape(block // 8, 8, queries), axis=0)
            acc_s[at] = acc_s[at] * fade + dot(
                v_s[h * head_width:(h + 1) * head_width, :], p.astype(jnp.bfloat16), (1, 0))

        highest = first_pass(0)
        for h in range(heads):
            following = first_pass(h + 1) if h + 1 < heads else None
            second_pass(h, highest)
            highest = following

    def attend_group(slot, k):
        theirs = lax.rem(group + k, groups)

        def one_block(b, carry):
            at = jnp.where(theirs > group, b, blocks - 1 - b) if k else b
            s0 = theirs * chips + at * pair
            if k:
                for i in range(pair):
                    await_source(slot, s0 + i)
            attend(slot, s0)
            return carry

        if not k:
            for c in range(chips):
                await_source(slot, theirs * chips + c)
            project_queries(slot)
        lax.fori_loop(0, blocks, one_block, 0)

    def units(slot):
        return [0] if slot == shared else list(range(m))

    def back(slot, u, c):
        hf = lat if slot == shared else u
        row = slot_row(slot)
        lon = group * chips + c
        copy = remote(mixed.at[slot, u, c], returned.at[row, hf], send2.at[slot, u, c], recv2.at[row, hf],
                      lon, source_lat)
        return row, hf, (lon != me) | (source_lat != lat), copy

    def hand_back(slot):
        for u in units(slot):
            for j in range(share):
                at = slot * HEADS + u * share + j
                done = (acc_s[at] / jnp.sum(sum_s[at], axis=0, keepdims=True)).astype(jnp.bfloat16)
                for c in range(chips):
                    mixed[slot, u, c, j * head_width:(j + 1) * head_width, :] = done[:, c * cells:(c + 1) * cells]
            for c in range(chips):
                row, hf, away, copy = back(slot, u, c)

                @pl.when(away)
                def _():
                    copy.start()

                @pl.when(jnp.logical_not(away))
                def _():
                    returned[row, hf] = mixed[slot, u, c]

    for k in range(groups):
        pass_on(k)
        for slot in (slots if not k else slots[::-1]):
            attend_group(slot, k)
            if k == groups - 1:
                hand_back(slot)

    for r in range(rows):
        w = r % rpc
        lon = group * chips + lat * per_lat + r // rpc
        for hf in range(m):
            core = 0 if w < full else 1 if w >= rpc - full else hf

            @pl.when((lon != me) | (core != lat))
            def _():
                remote(mixed.at[0, 0, 0], returned.at[r, hf], send2.at[0, 0, 0], recv2.at[r, hf], lon, core).wait_recv()
        att_t = returned[r].reshape(width, cells)
        update = dot(att_t, wout_ref[...], (0, 0))
        out_ref[r] = (fields_ref[r].astype(jnp.float32) + update).astype(jnp.bfloat16)

    each_forward(lambda copy: copy.wait_send())
    if shared is not None:
        for s in range(n):
            @pl.when((s != me) & (s % m == lat))
            def _():
                relay(s).wait_send()
    for slot in slots:
        for u in units(slot):
            for c in range(chips):
                row, hf, away, copy = back(slot, u, c)

                @pl.when(away)
                def _():
                    copy.wait_send()


def solution(mesh):
    n, m = mesh.shape["lon"], mesh.shape["lat"]

    def body(fields, norm_gain, w_qkv, w_out):
        rows, cells, width = fields.shape
        chips, rpc, full = plan(n, m, rows)
        groups, slots = n // chips, full + (1 if rpc % m else 0)
        queries, block = chips * cells, 2 * cells
        head_width = width // HEADS
        half = width // m
        bf16, f32 = jnp.bfloat16, jnp.float32
        return pl.pallas_call(
            functools.partial(kernel, n, m),
            out_shape=pltpu.VMEM(fields.shape, fields.dtype),
            in_specs=[pl.BlockSpec(memory_space=pltpu.HBM)] * 4,
            out_specs=pl.BlockSpec(memory_space=pltpu.VMEM),
            scratch_shapes=[
                pltpu.VMEM(fields.shape, fields.dtype),
                pltpu.VMEM((1, width), norm_gain.dtype),
                pltpu.VMEM(w_qkv.shape, w_qkv.dtype),
                pltpu.VMEM(w_out.shape, w_out.dtype),
                pltpu.VMEM((rows, cells, width), bf16),
                pltpu.VMEM((3 * width, width), bf16),
                pltpu.VMEM((slots, n, cells, width), bf16),
                pltpu.VMEM((block, queries), f32),
                pltpu.VMEM((block, queries), f32),
                pltpu.VMEM((slots, 2 * width, queries), bf16),
                pltpu.VMEM((block, 2 * width), bf16),
                pltpu.VMEM((width, block), bf16),
                pltpu.VMEM((slots * HEADS, 1, queries), f32),
                pltpu.VMEM((slots * HEADS, 8, queries), f32),
                pltpu.VMEM((slots * HEADS, head_width, queries), f32),
                pltpu.VMEM((slots, m, chips, half, cells), bf16),
                pltpu.VMEM((rows, m, half, cells), bf16),
                pltpu.SemaphoreType.DMA((4,)),
                pltpu.SemaphoreType.DMA((groups, rows)),
                pltpu.SemaphoreType.DMA((rows,)),
                pltpu.SemaphoreType.DMA((slots, n)),
                pltpu.SemaphoreType.DMA((n,)),
                pltpu.SemaphoreType.DMA((slots, m, chips)),
                pltpu.SemaphoreType.DMA((rows, m)),
            ],
            compiler_params=pltpu.CompilerParams(
                collective_id=0, has_side_effects=True, vmem_limit_bytes=40 * 2**20,
            ),
        )(*(
            pltpu.with_memory_space_constraint(x, pltpu.HBM)
            for x in (fields, norm_gain.reshape(1, width), w_qkv, w_out)
        ))

    return jax.shard_map(
        body,
        mesh=mesh,
        in_specs=(P(("groups", "lat"), "lon", None), P(), P(), P()),
        out_specs=P(("groups", "lat"), "lon", None),
        check_vma=False,
    )
```

```python
import functools
import math

import jax
import jax.numpy as jnp
from jax import lax
from jax.experimental import pallas as pl
from jax.experimental.pallas import tpu as pltpu
from jax.sharding import PartitionSpec as P

HEADS = 8
LOG2E = math.log2(math.e)
MESH = pl.DeviceIdType.MESH


def dot(a, b, contract):
    return lax.dot_general(a, b, ((contract[:1], contract[1:]), ((), ())), preferred_element_type=jnp.float32)


def plan(n, m, rows):
    chips = max(c for c in range(m, n // 2 + 1, m) if n % c == 0 and (rows * m) % c == 0)
    rpc = rows * m // chips
    return chips, rpc, rpc // m


def kernel(n, m, fields_hbm, gain_hbm, wqkv_hbm, wout_hbm, out_ref,
           fields_ref, gain_ref, wqkv_ref, wout_ref,
           normed, w_t, twice_s, x, scores_s, p_s, q_s, kk_s, v_s, top_s, sum_s, acc_s, mixed, returned,
           loaded, send1, twin1, recv1, relayed, send2, recv2, near, far):
    me, lat = lax.axis_index("lon"), lax.axis_index("lat")
    rows, cells, width = fields_ref.shape
    head_width = width // HEADS
    chips, rpc, full = plan(n, m, rows)
    groups = n // chips
    share = HEADS // m
    half = share * head_width
    queries = chips * cells
    pair = 2
    block = pair * cells
    blocks = chips // pair
    step = 32
    per_lat = chips // m
    group, chip = me // chips, lax.rem(me, chips)
    source_lat = chip // per_lat
    first_row = lax.rem(chip, per_lat) * rpc
    mine = source_lat == lat
    other = 1 - lat
    shared = full if rpc % m else None
    slots = list(range(full)) + ([full] if rpc % m else [])

    barrier = pltpu.get_barrier_semaphore()

    def greet(lon, core):
        pl.semaphore_signal(barrier, inc=1, device_id={"lon": lon, "lat": core}, device_id_type=MESH)

    for k in range(groups):
        for c in range(chips):
            lon = lax.rem(group + k, groups) * chips + c
            if k:
                greet(lon, m - 1)
            else:
                @pl.when((lon != me) | (lat != 0))
                def _():
                    greet(lon, 0)

    loads = [
        pltpu.make_async_copy(src, dst, loaded.at[i])
        for i, (src, dst) in enumerate((
            (fields_hbm, fields_ref), (gain_hbm, gain_ref), (wqkv_hbm, wqkv_ref), (wout_hbm, wout_ref),
        ))
    ]
    for load in loads:
        load.start()
    loads[1].wait()
    loads[0].wait()

    gain = gain_ref[...]
    for r in range(rows):
        inputs = fields_ref[r].astype(jnp.float32)
        center = jnp.mean(inputs, axis=-1, keepdims=True)
        spread = jnp.mean((inputs - center) ** 2, axis=-1, keepdims=True)
        normed[r] = ((inputs - center) * lax.rsqrt(spread + 1e-05) * gain).astype(jnp.bfloat16)

    loads[2].wait()
    loads[3].wait()
    w_t[...] = wqkv_ref[...].astype(jnp.float32).T.astype(jnp.bfloat16)
    for g in range(m):
        w_k = w_t[width + g * half:width + (g + 1) * half, :]
        twice_s[0, g] = jnp.concatenate([w_k, w_k], axis=0)
    twice_s[1, 0] = twice_s[0, lat]
    top_s[...] = jnp.full(top_s.shape, -jnp.inf, jnp.float32)
    sum_s[...] = jnp.zeros(sum_s.shape, jnp.float32)
    acc_s[...] = jnp.zeros(acc_s.shape, jnp.float32)

    def slot_row(slot):
        if slot == shared:
            return first_row + full
        return first_row + slot + lat * (rpc - full)

    def remote(src, dst, send, recv, lon, core):
        return pltpu.make_async_remote_copy(
            src_ref=src, dst_ref=dst, send_sem=send, recv_sem=recv,
            device_id={"lon": lon, "lat": core}, device_id_type=MESH)

    def forward(k, r):
        lon = lax.rem(group + k, groups) * chips + lat * per_lat + r // rpc
        w = r % rpc
        if w < full:
            slot, core = w, 0
        elif w >= rpc - full:
            slot, core = w - (rpc - full), 1
        else:
            slot, core = full, lax.rem(me, m)
        away = True if k else (lon != me)
        if not k and slot != shared:
            away = (lon != me) | (core != lat)
        copy = remote(normed.at[r], x.at[slot, me], send1.at[k, r], recv1.at[slot, me], lon, core)
        twin = None
        if not k and slot == shared:
            twin = remote(normed.at[r], x.at[slot, me], twin1.at[r], recv1.at[slot, me], me, other)
        return slot, away, copy, twin

    order = [r for r in range(rows) if full <= r % rpc < rpc - full] + [
        r for r in range(rows) if not full <= r % rpc < rpc - full]

    def each_forward(use, ks):
        for k in ks:
            for r in order:
                slot, away, copy, twin = forward(k, r)
                if away is True:
                    use(copy)
                    continue

                @pl.when(away)
                def _():
                    use(copy)

                if twin is not None:
                    @pl.when(jnp.logical_not(away))
                    def _():
                        use(twin)

    @pl.when(lat == 0)
    def _():
        pl.semaphore_wait(barrier, chips * m - 1)
        pl.semaphore_signal(near, inc=1, device_id={"lon": me, "lat": 1}, device_id_type=MESH)

    @pl.when(lat != 0)
    def _():
        pl.semaphore_wait(near, 1)

    each_forward(lambda copy: copy.start(), [0])

    @pl.when(lat != 0)
    def _():
        pl.semaphore_wait(barrier, (n - chips) * m)
        pl.semaphore_signal(far, inc=1, device_id={"lon": me, "lat": 0}, device_id_type=MESH)

    @pl.when(lat == 0)
    def _():
        pl.semaphore_wait(far, 1)

    each_forward(lambda copy: copy.start(), range(1, groups))

    @pl.when(mine)
    def _():
        for slot in slots:
            x[slot, me] = normed[slot_row(slot)]

    def arrival(slot, s):
        return remote(normed.at[0], x.at[slot, s], send1.at[0, 0], recv1.at[slot, s], s, lat)

    def relay(s):
        return remote(x.at[full, s], x.at[full, s], relayed.at[s], recv1.at[full, s], me, other)

    def pass_on(k):
        if shared is None:
            return
        for c in range(chips):
            s = lax.rem(group + k, groups) * chips + c

            @pl.when((s != me) & (lax.rem(s, m) == lat))
            def _():
                arrival(full, s).wait_recv()
                relay(s).start()

    def weight(part, slot):
        start = part * width
        if slot != shared:
            return w_t[start:start + width, :]
        return w_t[pl.ds(pl.multiple_of(start + lat * half, half), half), :]

    def await_source(slot, s):
        if slot == shared:
            due = jnp.where(s == me, jnp.logical_not(mine), lax.rem(s, m) != lat)
        else:
            due = (s != me) | jnp.logical_not(mine)

        @pl.when(due)
        def _():
            arrival(slot, s).wait_recv()

    def heads_of(slot):
        return share if slot == shared else HEADS

    def project_queries(slot):
        span = heads_of(slot) * head_width
        for b in range(blocks):
            cell_rows = x[slot, pl.ds(group * chips + b * pair, pair)].reshape(block, width)
            q_t = (dot(weight(0, slot), cell_rows, (1, 1)) * (1.0 / math.sqrt(head_width))).astype(jnp.bfloat16)
            q_t = q_t.astype(jnp.float32) * LOG2E
            q_hi = q_t.astype(jnp.bfloat16)
            q_lo = (q_t - q_hi.astype(jnp.float32)).astype(jnp.bfloat16)
            q_s[slot, 0:span, b * block:(b + 1) * block] = q_hi
            q_s[slot, width:width + span, b * block:(b + 1) * block] = q_lo

    def attend(slot, s0):
        heads = heads_of(slot)
        cell_rows = x[slot, pl.ds(s0, pair)].reshape(block, width)
        for g in range(heads // share):
            kk_s[g] = dot(cell_rows, twice_s[int(slot == shared), g], (1, 1)).astype(jnp.bfloat16)
        v_s[0:heads * head_width, :] = dot(weight(2, slot), cell_rows, (1, 1)).astype(jnp.bfloat16)

        def gap(size):
            return [jnp.zeros((size, queries), jnp.bfloat16)] if size else []

        def scores(h):
            g, at = h // share, h % share * head_width
            lo, hi = h * head_width, (h + 1) * head_width
            before, after = gap(at), gap(half - head_width - at)
            spread_q = jnp.concatenate(
                before + [q_s[slot, lo:hi, :]] + after + before + [q_s[slot, width + lo:width + hi, :]] + after, axis=0)
            return dot(kk_s[g], spread_q, (1, 0))

        def keep(h, s, c, part):
            piece = s[c * step:(c + 1) * step]
            scores_s[h % 2, c * step:(c + 1) * step, :] = piece
            part_max = jnp.max(piece.reshape(step // 8, 8, queries), axis=0)
            return part_max if part is None else jnp.maximum(part, part_max)

        def weigh(h, fade):
            at = slot * HEADS + h
            acc_s[at] = acc_s[at] * fade + dot(v_s[h * head_width:(h + 1) * head_width, :], p_s[h % 2], (1, 0))

        s, part = scores(0), None
        for c in range(block // step):
            part = keep(0, s, c, part)
        fades = {}
        for h in range(heads):
            highest = jnp.max(part, axis=0, keepdims=True)
            s = scores(h + 1) if h + 1 < heads else None
            if h:
                weigh(h - 1, fades[h - 1])
            at = slot * HEADS + h
            before = top_s[at]
            now = jnp.maximum(before, highest)
            fades[h] = jnp.exp2(before - now)
            top_s[at] = now
            part = total = None
            for c in range(block // step):
                p = jnp.exp2(scores_s[h % 2, c * step:(c + 1) * step, :] - now)
                piece = jnp.sum(p.reshape(step // 8, 8, queries), axis=0)
                total = piece if total is None else total + piece
                p_s[h % 2, c * step:(c + 1) * step, :] = p.astype(jnp.bfloat16)
                if s is not None:
                    part = keep(h + 1, s, c, part)
            sum_s[at] = sum_s[at] * fades[h] + total
        weigh(heads - 1, fades[heads - 1])

    def attend_group(slot, k):
        theirs = lax.rem(group + k, groups)

        def one_block(b, carry):
            at = jnp.where(theirs > group, b, blocks - 1 - b) if k else b
            s0 = theirs * chips + at * pair
            if k:
                for i in range(pair):
                    await_source(slot, s0 + i)
            attend(slot, s0)
            return carry

        if not k:
            for c in range(chips):
                await_source(slot, theirs * chips + c)
            project_queries(slot)
        lax.fori_loop(0, blocks, one_block, 0)

    def units(slot):
        return [0] if slot == shared else list(range(m))

    def back(slot, u, c):
        hf = lat if slot == shared else u
        row = slot_row(slot)
        lon = group * chips + c
        copy = remote(mixed.at[slot, u, c], returned.at[row, hf], send2.at[slot, u, c], recv2.at[row, hf],
                      lon, source_lat)
        return row, hf, (lon != me) | (source_lat != lat), copy

    def hand_back(slot):
        for u in units(slot):
            for j in range(share):
                at = slot * HEADS + u * share + j
                done = (acc_s[at] / jnp.sum(sum_s[at], axis=0, keepdims=True)).astype(jnp.bfloat16)
                for c in range(chips):
                    mixed[slot, u, c, j * head_width:(j + 1) * head_width, :] = done[:, c * cells:(c + 1) * cells]
            for c in range(chips):
                row, hf, away, copy = back(slot, u, c)

                @pl.when(away)
                def _():
                    copy.start()

                @pl.when(jnp.logical_not(away))
                def _():
                    returned[row, hf] = mixed[slot, u, c]

    for k in range(groups):
        pass_on(k)
        for slot in (slots if not k else slots[::-1]):
            attend_group(slot, k)
            if k == groups - 1:
                hand_back(slot)

    for r in range(rows):
        w = r % rpc
        lon = group * chips + lat * per_lat + r // rpc
        for hf in range(m):
            core = 0 if w < full else 1 if w >= rpc - full else hf

            @pl.when((lon != me) | (core != lat))
            def _():
                remote(mixed.at[0, 0, 0], returned.at[r, hf], send2.at[0, 0, 0], recv2.at[r, hf], lon, core).wait_recv()
        att_t = returned[r].reshape(width, cells)
        update = dot(att_t, wout_ref[...], (0, 0))
        out_ref[r] = (fields_ref[r].astype(jnp.float32) + update).astype(jnp.bfloat16)

    each_forward(lambda copy: copy.wait_send(), range(groups))
    if shared is not None:
        for s in range(n):
            @pl.when((s != me) & (s % m == lat))
            def _():
                relay(s).wait_send()
    for slot in slots:
        for u in units(slot):
            for c in range(chips):
                row, hf, away, copy = back(slot, u, c)

                @pl.when(away)
                def _():
                    copy.wait_send()


def solution(mesh):
    n, m = mesh.shape["lon"], mesh.shape["lat"]

    def body(fields, norm_gain, w_qkv, w_out):
        rows, cells, width = fields.shape
        chips, rpc, full = plan(n, m, rows)
        groups, slots = n // chips, full + (1 if rpc % m else 0)
        queries, block = chips * cells, 2 * cells
        head_width = width // HEADS
        half = width // m
        bf16, f32 = jnp.bfloat16, jnp.float32
        return pl.pallas_call(
            functools.partial(kernel, n, m),
            out_shape=pltpu.VMEM(fields.shape, fields.dtype),
            in_specs=[pl.BlockSpec(memory_space=pltpu.HBM)] * 4,
            out_specs=pl.BlockSpec(memory_space=pltpu.VMEM),
            scratch_shapes=[
                pltpu.VMEM(fields.shape, fields.dtype),
                pltpu.VMEM((1, width), norm_gain.dtype),
                pltpu.VMEM(w_qkv.shape, w_qkv.dtype),
                pltpu.VMEM(w_out.shape, w_out.dtype),
                pltpu.VMEM((rows, cells, width), bf16),
                pltpu.VMEM((3 * width, width), bf16),
                pltpu.VMEM((2, m, 2 * half, width), bf16),
                pltpu.VMEM((slots, n, cells, width), bf16),
                pltpu.VMEM((2, block, queries), f32),
                pltpu.VMEM((2, block, queries), bf16),
                pltpu.VMEM((slots, 2 * width, queries), bf16),
                pltpu.VMEM((m, block, 2 * half), bf16),
                pltpu.VMEM((width, block), bf16),
                pltpu.VMEM((slots * HEADS, 1, queries), f32),
                pltpu.VMEM((slots * HEADS, 8, queries), f32),
                pltpu.VMEM((slots * HEADS, head_width, queries), f32),
                pltpu.VMEM((slots, m, chips, half, cells), bf16),
                pltpu.VMEM((rows, m, half, cells), bf16),
                pltpu.SemaphoreType.DMA((4,)),
                pltpu.SemaphoreType.DMA((groups, rows)),
                pltpu.SemaphoreType.DMA((rows,)),
                pltpu.SemaphoreType.DMA((slots, n)),
                pltpu.SemaphoreType.DMA((n,)),
                pltpu.SemaphoreType.DMA((slots, m, chips)),
                pltpu.SemaphoreType.DMA((rows, m)),
                pltpu.SemaphoreType.REGULAR,
                pltpu.SemaphoreType.REGULAR,
            ],
            compiler_params=pltpu.CompilerParams(
                collective_id=0, has_side_effects=True, vmem_limit_bytes=40 * 2**20,
            ),
        )(*(
            pltpu.with_memory_space_constraint(x, pltpu.HBM)
            for x in (fields, norm_gain.reshape(1, width), w_qkv, w_out)
        ))

    return jax.shard_map(
        body,
        mesh=mesh,
        in_specs=(P(("groups", "lat"), "lon", None), P(), P(), P()),
        out_specs=P(("groups", "lat"), "lon", None),
        check_vma=False,
    )
```

```python
import functools
import math

import jax
import jax.numpy as jnp
from jax import lax
from jax.experimental import pallas as pl
from jax.experimental.pallas import tpu as pltpu
from jax.sharding import PartitionSpec as P

HEADS = 8
TILE = 256
LOG2E = math.log2(math.e)
MESH = pl.DeviceIdType.MESH


def dot(a, b, contract):
    return lax.dot_general(a, b, ((contract[:1], contract[1:]), ((), ())), preferred_element_type=jnp.float32)


def plan(n, m, rows):
    chips = max(c for c in range(m, n // 2 + 1, m) if n % c == 0 and (rows * m) % c == 0)
    rpc = rows * m // chips
    return chips, rpc, rpc // m


def kernel(n, m, fields_hbm, gain_hbm, wqkv_hbm, wout_hbm, out_ref,
           fields_ref, gain_ref, wqkv_ref, wout_ref,
           normed, w_t, twice_s, x, scores_s, p_s, q_s, kk_s, v_s, top_s, sum_s, acc_s, mixed, returned,
           loaded, send1, twin1, recv1, relayed, send2, recv2, near, far):
    me, lat = lax.axis_index("lon"), lax.axis_index("lat")
    rows, cells, width = fields_ref.shape
    head_width = width // HEADS
    chips, rpc, full = plan(n, m, rows)
    groups = n // chips
    share = HEADS // m
    half = share * head_width
    queries = chips * cells
    pair = 2
    block = pair * cells
    blocks = chips // pair
    step = 32
    per_lat = chips // m
    group, chip = me // chips, lax.rem(me, chips)
    source_lat = chip // per_lat
    first_row = lax.rem(chip, per_lat) * rpc
    mine = source_lat == lat
    other = 1 - lat
    shared = full if rpc % m else None
    slots = list(range(full)) + ([full] if rpc % m else [])

    barrier = pltpu.get_barrier_semaphore()

    def greet(lon, core):
        pl.semaphore_signal(barrier, inc=1, device_id={"lon": lon, "lat": core}, device_id_type=MESH)

    for k in range(groups):
        for c in range(chips):
            lon = lax.rem(group + k, groups) * chips + c
            if k:
                greet(lon, m - 1)
            else:
                @pl.when((lon != me) | (lat != 0))
                def _():
                    greet(lon, 0)

    loads = [
        pltpu.make_async_copy(src, dst, loaded.at[i])
        for i, (src, dst) in enumerate((
            (fields_hbm, fields_ref), (gain_hbm, gain_ref), (wqkv_hbm, wqkv_ref), (wout_hbm, wout_ref),
        ))
    ]
    for load in loads:
        load.start()
    loads[1].wait()
    loads[0].wait()

    gain = gain_ref[...]
    for r in range(rows):
        inputs = fields_ref[r].astype(jnp.float32)
        center = jnp.mean(inputs, axis=-1, keepdims=True)
        spread = jnp.mean((inputs - center) ** 2, axis=-1, keepdims=True)
        normed[r] = ((inputs - center) * lax.rsqrt(spread + 1e-05) * gain).astype(jnp.bfloat16)

    loads[2].wait()
    loads[3].wait()
    w_t[...] = wqkv_ref[...].astype(jnp.float32).T.astype(jnp.bfloat16)
    for g in range(m):
        w_k = w_t[width + g * half:width + (g + 1) * half, :]
        twice_s[0, g] = jnp.concatenate([w_k, w_k], axis=0)
    twice_s[1, 0] = twice_s[0, lat]
    top_s[...] = jnp.full(top_s.shape, -jnp.inf, jnp.float32)
    sum_s[...] = jnp.zeros(sum_s.shape, jnp.float32)
    acc_s[...] = jnp.zeros(acc_s.shape, jnp.float32)

    def slot_row(slot):
        if slot == shared:
            return first_row + full
        return first_row + slot + lat * (rpc - full)

    def remote(src, dst, send, recv, lon, core):
        return pltpu.make_async_remote_copy(
            src_ref=src, dst_ref=dst, send_sem=send, recv_sem=recv,
            device_id={"lon": lon, "lat": core}, device_id_type=MESH)

    def forward(k, r):
        lon = lax.rem(group + k, groups) * chips + lat * per_lat + r // rpc
        w = r % rpc
        if w < full:
            slot, core = w, 0
        elif w >= rpc - full:
            slot, core = w - (rpc - full), 1
        else:
            slot, core = full, lax.rem(me, m)
        away = True if k else (lon != me)
        if not k and slot != shared:
            away = (lon != me) | (core != lat)
        copy = remote(normed.at[r], x.at[slot, me], send1.at[k, r], recv1.at[slot, me], lon, core)
        twin = None
        if not k and slot == shared:
            twin = remote(normed.at[r], x.at[slot, me], twin1.at[r], recv1.at[slot, me], me, other)
        return slot, away, copy, twin

    order = [r for r in range(rows) if full <= r % rpc < rpc - full] + [
        r for r in range(rows) if not full <= r % rpc < rpc - full]

    def each_forward(use, ks):
        for k in ks:
            for r in order:
                slot, away, copy, twin = forward(k, r)
                if away is True:
                    use(copy)
                    continue

                @pl.when(away)
                def _():
                    use(copy)

                if twin is not None:
                    @pl.when(jnp.logical_not(away))
                    def _():
                        use(twin)

    @pl.when(lat == 0)
    def _():
        pl.semaphore_wait(barrier, chips * m - 1)
        pl.semaphore_signal(near, inc=1, device_id={"lon": me, "lat": 1}, device_id_type=MESH)

    @pl.when(lat != 0)
    def _():
        pl.semaphore_wait(near, 1)

    each_forward(lambda copy: copy.start(), [0])

    @pl.when(lat != 0)
    def _():
        pl.semaphore_wait(barrier, (n - chips) * m)
        pl.semaphore_signal(far, inc=1, device_id={"lon": me, "lat": 0}, device_id_type=MESH)

    @pl.when(lat == 0)
    def _():
        pl.semaphore_wait(far, 1)

    each_forward(lambda copy: copy.start(), range(1, groups))

    @pl.when(mine)
    def _():
        for slot in slots:
            x[slot, me] = normed[slot_row(slot)]

    def arrival(slot, s):
        return remote(normed.at[0], x.at[slot, s], send1.at[0, 0], recv1.at[slot, s], s, lat)

    def relay(s):
        return remote(x.at[full, s], x.at[full, s], relayed.at[s], recv1.at[full, s], me, other)

    def pass_on(k):
        if shared is None:
            return
        for c in range(chips):
            s = lax.rem(group + k, groups) * chips + c

            @pl.when((s != me) & (lax.rem(s, m) == lat))
            def _():
                arrival(full, s).wait_recv()
                relay(s).start()

    def weight(part, slot):
        start = part * width
        if slot != shared:
            return w_t[start:start + width, :]
        return w_t[pl.ds(pl.multiple_of(start + lat * half, half), half), :]

    def await_source(slot, s):
        if slot == shared:
            due = jnp.where(s == me, jnp.logical_not(mine), lax.rem(s, m) != lat)
        else:
            due = (s != me) | jnp.logical_not(mine)

        @pl.when(due)
        def _():
            arrival(slot, s).wait_recv()

    def heads_of(slot):
        return share if slot == shared else HEADS

    def project_queries(slot):
        span = heads_of(slot) * head_width
        for b in range(blocks):
            cell_rows = x[slot, pl.ds(group * chips + b * pair, pair)].reshape(block, width)
            q_t = (dot(weight(0, slot), cell_rows, (1, 1)) * (1.0 / math.sqrt(head_width))).astype(jnp.bfloat16)
            q_t = q_t.astype(jnp.float32) * LOG2E
            q_hi = q_t.astype(jnp.bfloat16)
            q_lo = (q_t - q_hi.astype(jnp.float32)).astype(jnp.bfloat16)
            q_s[slot, 0:span, b * block:(b + 1) * block] = q_hi
            q_s[slot, width:width + span, b * block:(b + 1) * block] = q_lo

    def units(slot):
        return [0] if slot == shared else list(range(m))

    def prepare(slot, b, s0):
        cell_rows = x[slot, pl.ds(s0, pair)].reshape(block, width)
        for u in units(slot):
            kk_s[slot, u, b * block:(b + 1) * block, :] = dot(
                cell_rows, twice_s[int(slot == shared), u], (1, 1)).astype(jnp.bfloat16)
        v_s[slot, 0:heads_of(slot) * head_width, b * block:(b + 1) * block] = dot(
            weight(2, slot), cell_rows, (1, 1)).astype(jnp.bfloat16)

    def gap(size):
        return [jnp.zeros((size, queries), jnp.bfloat16)] if size else []

    def attend(items):
        def scores(slot, h, first, size):
            u, at = h // share, h % share * head_width
            lo, hi = h * head_width, (h + 1) * head_width
            before, after = gap(at), gap(half - head_width - at)
            spread_q = jnp.concatenate(
                before + [q_s[slot, lo:hi, :]] + after + before + [q_s[slot, width + lo:width + hi, :]] + after, axis=0)
            return dot(kk_s[slot, u, first:first + size, :], spread_q, (1, 0))

        def keep(i, s, c, part):
            piece = s[c * step:(c + 1) * step]
            scores_s[i % 2, c * step:(c + 1) * step, :] = piece
            part_max = jnp.max(piece.reshape(step // 8, 8, queries), axis=0)
            return part_max if part is None else jnp.maximum(part, part_max)

        def weigh(i, fade):
            slot, h, first, size = items[i]
            at = slot * HEADS + h
            acc_s[at] = acc_s[at] * fade + dot(
                v_s[slot, h * head_width:(h + 1) * head_width, first:first + size], p_s[i % 2, 0:size], (1, 0))

        s, part = scores(*items[0]), None
        for c in range(items[0][3] // step):
            part = keep(0, s, c, part)
        fade = None
        for i, (slot, h, first, size) in enumerate(items):
            highest = jnp.max(part, axis=0, keepdims=True)
            s = scores(*items[i + 1]) if i + 1 < len(items) else None
            if i:
                weigh(i - 1, fade)
            at = slot * HEADS + h
            before = top_s[at]
            now = jnp.maximum(before, highest)
            fade = jnp.exp2(before - now)
            top_s[at] = now
            part = total = None
            for c in range(size // step):
                p = jnp.exp2(scores_s[i % 2, c * step:(c + 1) * step, :] - now)
                piece = jnp.sum(p.reshape(step // 8, 8, queries), axis=0)
                total = piece if total is None else total + piece
                p_s[i % 2, c * step:(c + 1) * step, :] = p.astype(jnp.bfloat16)
                if s is not None:
                    part = keep(i + 1, s, c, part)
            sum_s[at] = sum_s[at] * fade + total
        weigh(len(items) - 1, fade)

    def await_group(slot, k):
        for c in range(chips):
            await_source(slot, lax.rem(group + k, groups) * chips + c)

    def prepare_group(slot, k):
        for b in range(blocks):
            prepare(slot, b, lax.rem(group + k, groups) * chips + b * pair)

    def unit_items(slot, u):
        wide = min(TILE, queries)
        return [(slot, u * share + h, first, wide) for first in range(0, queries, wide) for h in range(share)]

    def back(slot, u, c):
        hf = lat if slot == shared else u
        row = slot_row(slot)
        lon = group * chips + c
        copy = remote(mixed.at[slot, u, c], returned.at[row, hf], send2.at[slot, u, c], recv2.at[row, hf],
                      lon, source_lat)
        return row, hf, (lon != me) | (source_lat != lat), copy

    def hand_back(slot, u):
        for j in range(share):
            at = slot * HEADS + u * share + j
            done = (acc_s[at] / jnp.sum(sum_s[at], axis=0, keepdims=True)).astype(jnp.bfloat16)
            for c in range(chips):
                mixed[slot, u, c, j * head_width:(j + 1) * head_width, :] = done[:, c * cells:(c + 1) * cells]
        for c in range(chips):
            row, hf, away, copy = back(slot, u, c)

            @pl.when(away)
            def _():
                copy.start()

            @pl.when(jnp.logical_not(away))
            def _():
                returned[row, hf] = mixed[slot, u, c]

    pass_on(0)
    for slot in slots:
        await_group(slot, 0)
        project_queries(slot)
        prepare_group(slot, 0)
        attend([item for u in units(slot) for item in unit_items(slot, u)])
    for k in range(1, groups):
        pass_on(k)
        for slot in slots[::-1]:
            await_group(slot, k)
            prepare_group(slot, k)
            for u in units(slot):
                attend(unit_items(slot, u))
                if k == groups - 1:
                    hand_back(slot, u)

    for r in range(rows):
        w = r % rpc
        lon = group * chips + lat * per_lat + r // rpc
        for hf in range(m):
            core = 0 if w < full else 1 if w >= rpc - full else hf

            @pl.when((lon != me) | (core != lat))
            def _():
                remote(mixed.at[0, 0, 0], returned.at[r, hf], send2.at[0, 0, 0], recv2.at[r, hf], lon, core).wait_recv()
        att_t = returned[r].reshape(width, cells)
        update = dot(att_t, wout_ref[...], (0, 0))
        out_ref[r] = (fields_ref[r].astype(jnp.float32) + update).astype(jnp.bfloat16)

    each_forward(lambda copy: copy.wait_send(), range(groups))
    if shared is not None:
        for s in range(n):
            @pl.when((s != me) & (s % m == lat))
            def _():
                relay(s).wait_send()
    for slot in slots:
        for u in units(slot):
            for c in range(chips):
                row, hf, away, copy = back(slot, u, c)

                @pl.when(away)
                def _():
                    copy.wait_send()


def solution(mesh):
    n, m = mesh.shape["lon"], mesh.shape["lat"]

    def body(fields, norm_gain, w_qkv, w_out):
        rows, cells, width = fields.shape
        chips, rpc, full = plan(n, m, rows)
        groups, slots = n // chips, full + (1 if rpc % m else 0)
        queries, block = chips * cells, 2 * cells
        head_width = width // HEADS
        half = width // m
        bf16, f32 = jnp.bfloat16, jnp.float32
        return pl.pallas_call(
            functools.partial(kernel, n, m),
            out_shape=pltpu.VMEM(fields.shape, fields.dtype),
            in_specs=[pl.BlockSpec(memory_space=pltpu.HBM)] * 4,
            out_specs=pl.BlockSpec(memory_space=pltpu.VMEM),
            scratch_shapes=[
                pltpu.VMEM(fields.shape, fields.dtype),
                pltpu.VMEM((1, width), norm_gain.dtype),
                pltpu.VMEM(w_qkv.shape, w_qkv.dtype),
                pltpu.VMEM(w_out.shape, w_out.dtype),
                pltpu.VMEM((rows, cells, width), bf16),
                pltpu.VMEM((3 * width, width), bf16),
                pltpu.VMEM((2, m, 2 * half, width), bf16),
                pltpu.VMEM((slots, n, cells, width), bf16),
                pltpu.VMEM((2, min(TILE, queries), queries), f32),
                pltpu.VMEM((2, min(TILE, queries), queries), bf16),
                pltpu.VMEM((slots, 2 * width, queries), bf16),
                pltpu.VMEM((slots, m, queries, 2 * half), bf16),
                pltpu.VMEM((slots, width, queries), bf16),
                pltpu.VMEM((slots * HEADS, 1, queries), f32),
                pltpu.VMEM((slots * HEADS, 8, queries), f32),
                pltpu.VMEM((slots * HEADS, head_width, queries), f32),
                pltpu.VMEM((slots, m, chips, half, cells), bf16),
                pltpu.VMEM((rows, m, half, cells), bf16),
                pltpu.SemaphoreType.DMA((4,)),
                pltpu.SemaphoreType.DMA((groups, rows)),
                pltpu.SemaphoreType.DMA((rows,)),
                pltpu.SemaphoreType.DMA((slots, n)),
                pltpu.SemaphoreType.DMA((n,)),
                pltpu.SemaphoreType.DMA((slots, m, chips)),
                pltpu.SemaphoreType.DMA((rows, m)),
                pltpu.SemaphoreType.REGULAR,
                pltpu.SemaphoreType.REGULAR,
            ],
            compiler_params=pltpu.CompilerParams(
                collective_id=0, has_side_effects=True, vmem_limit_bytes=40 * 2**20,
            ),
        )(*(
            pltpu.with_memory_space_constraint(x, pltpu.HBM)
            for x in (fields, norm_gain.reshape(1, width), w_qkv, w_out)
        ))

    return jax.shard_map(
        body,
        mesh=mesh,
        in_specs=(P(("groups", "lat"), "lon", None), P(), P(), P()),
        out_specs=P(("groups", "lat"), "lon", None),
        check_vma=False,
    )
```

```python
import functools
import math

import jax
import jax.numpy as jnp
from jax import lax
from jax.experimental import pallas as pl
from jax.experimental.pallas import tpu as pltpu
from jax.sharding import PartitionSpec as P

HEADS = 8
TILE = 256
LOG2E = math.log2(math.e)
MESH = pl.DeviceIdType.MESH


def dot(a, b, contract):
    return lax.dot_general(a, b, ((contract[:1], contract[1:]), ((), ())), preferred_element_type=jnp.float32)


def plan(n, m, rows):
    chips = max(c for c in range(m, n // 2 + 1, m) if n % c == 0 and (rows * m) % c == 0)
    rpc = rows * m // chips
    return chips, rpc, rpc // m


def kernel(n, m, fields_hbm, gain_hbm, wqkv_hbm, wout_hbm, out_ref,
           fields_ref, gain_ref, wqkv_ref, wout_ref,
           normed, w_t, twice_s, x, scores_s, p_s, q_s, kk_s, v_s, top_s, sum_s, acc_s, mixed, returned,
           loaded, send1, twin1, recv1, relayed, send2, recv2, near, far, deep):
    me, lat = lax.axis_index("lon"), lax.axis_index("lat")
    rows, cells, width = fields_ref.shape
    head_width = width // HEADS
    chips, rpc, full = plan(n, m, rows)
    groups = n // chips
    share = HEADS // m
    half = share * head_width
    queries = chips * cells
    pair = 2
    block = pair * cells
    blocks = chips // pair
    step = 32
    per_lat = chips // m
    group, chip = me // chips, lax.rem(me, chips)
    source_lat = chip // per_lat
    first_row = lax.rem(chip, per_lat) * rpc
    mine = source_lat == lat
    other = 1 - lat
    shared = full if rpc % m else None
    slots = list(range(full)) + ([full] if rpc % m else [])

    barrier = pltpu.get_barrier_semaphore()

    def greet(lon, core):
        pl.semaphore_signal(barrier, inc=1, device_id={"lon": lon, "lat": core}, device_id_type=MESH)

    relayed_word = groups == 2 and m == 2 and per_lat == pair
    at_border = chip // pair == 1 - group
    outward = pair * (2 * group - 1)
    for k in range(groups):
        for c in range(chips):
            lon = lax.rem(group + k, groups) * chips + c
            if k and relayed_word:
                @pl.when(at_border)
                def _():
                    greet(lon, m - 1)
            elif k:
                greet(lon, m - 1)
            else:
                @pl.when((lon != me) | (lat != 0))
                def _():
                    greet(lon, 0)

    loads = [
        pltpu.make_async_copy(src, dst, loaded.at[i])
        for i, (src, dst) in enumerate((
            (fields_hbm, fields_ref), (gain_hbm, gain_ref), (wqkv_hbm, wqkv_ref), (wout_hbm, wout_ref),
        ))
    ]
    for load in loads:
        load.start()
    loads[1].wait()
    loads[0].wait()

    gain = gain_ref[...]
    for r in range(rows):
        inputs = fields_ref[r].astype(jnp.float32)
        center = jnp.mean(inputs, axis=-1, keepdims=True)
        spread = jnp.mean((inputs - center) ** 2, axis=-1, keepdims=True)
        normed[r] = ((inputs - center) * lax.rsqrt(spread + 1e-05) * gain).astype(jnp.bfloat16)

    def slot_row(slot):
        if slot == shared:
            return first_row + full
        return first_row + slot + lat * (rpc - full)

    def remote(src, dst, send, recv, lon, core):
        return pltpu.make_async_remote_copy(
            src_ref=src, dst_ref=dst, send_sem=send, recv_sem=recv,
            device_id={"lon": lon, "lat": core}, device_id_type=MESH)

    def forward(k, r):
        lon = lax.rem(group + k, groups) * chips + lat * per_lat + r // rpc
        w = r % rpc
        if w < full:
            slot, core = w, 0
        elif w >= rpc - full:
            slot, core = w - (rpc - full), 1
        else:
            slot, core = full, lax.rem(me, m)
        away = True if k else (lon != me)
        if not k and slot != shared:
            away = (lon != me) | (core != lat)
        copy = remote(normed.at[r], x.at[slot, me], send1.at[k, r], recv1.at[slot, me], lon, core)
        twin = None
        if not k and slot == shared:
            twin = remote(normed.at[r], x.at[slot, me], twin1.at[r], recv1.at[slot, me], me, other)
        return slot, away, copy, twin

    order = [r for r in range(rows) if full <= r % rpc < rpc - full] + [
        r for r in range(rows) if not full <= r % rpc < rpc - full]

    cross_order = sorted(order, key=lambda r: (order.index(r) >= rows // rpc, r % rpc, -r))

    def each_forward(use, ks):
        for k in ks:
            for r in (cross_order if k else order):
                slot, away, copy, twin = forward(k, r)
                if away is True:
                    use(copy)
                    continue

                @pl.when(away)
                def _():
                    use(copy)

                if twin is not None:
                    @pl.when(jnp.logical_not(away))
                    def _():
                        use(twin)

    @pl.when(lat == 0)
    def _():
        pl.semaphore_wait(barrier, chips * m - 1)
        pl.semaphore_signal(near, inc=1, device_id={"lon": me, "lat": 1}, device_id_type=MESH)

    @pl.when(lat != 0)
    def _():
        pl.semaphore_wait(near, 1)

    each_forward(lambda copy: copy.start(), [0])

    @pl.when(lat != 0)
    def _():
        pl.semaphore_wait(barrier, pair * m if relayed_word else (n - chips) * m)
        pl.semaphore_signal(far, inc=1, device_id={"lon": me, "lat": 0}, device_id_type=MESH)
        if relayed_word:
            @pl.when(at_border)
            def _():
                pl.semaphore_signal(
                    deep, inc=1, device_id={"lon": (1 - group) * chips + chip + outward, "lat": group}, device_id_type=MESH)

    @pl.when(lat == 0)
    def _():
        pl.semaphore_wait(far, 1)

    if relayed_word:
        @pl.when(lat != group)
        def _():
            pl.semaphore_wait(deep, 1)

            @pl.when(at_border)
            def _():
                pl.semaphore_signal(deep, inc=1, device_id={"lon": me + outward, "lat": lat}, device_id_type=MESH)

    each_forward(lambda copy: copy.start(), range(1, groups))

    loads[2].wait()
    loads[3].wait()
    w_t[...] = wqkv_ref[...].astype(jnp.float32).T.astype(jnp.bfloat16)
    for g in range(m):
        w_k = w_t[width + g * half:width + (g + 1) * half, :]
        twice_s[0, g] = jnp.concatenate([w_k, w_k], axis=0)
    twice_s[1, 0] = twice_s[0, lat]
    top_s[...] = jnp.full(top_s.shape, -jnp.inf, jnp.float32)
    sum_s[...] = jnp.zeros(sum_s.shape, jnp.float32)
    acc_s[...] = jnp.zeros(acc_s.shape, jnp.float32)

    @pl.when(mine)
    def _():
        for slot in slots:
            x[slot, me] = normed[slot_row(slot)]

    def arrival(slot, s):
        return remote(normed.at[0], x.at[slot, s], send1.at[0, 0], recv1.at[slot, s], s, lat)

    def relay(s):
        return remote(x.at[full, s], x.at[full, s], relayed.at[s], recv1.at[full, s], me, other)

    def pass_on(k):
        if shared is None:
            return
        for c in range(chips):
            s = lax.rem(group + k, groups) * chips + c

            @pl.when((s != me) & (lax.rem(s, m) == lat))
            def _():
                arrival(full, s).wait_recv()
                relay(s).start()

    def weight(part, slot):
        start = part * width
        if slot != shared:
            return w_t[start:start + width, :]
        return w_t[pl.ds(pl.multiple_of(start + lat * half, half), half), :]

    def await_source(slot, s):
        if slot == shared:
            due = jnp.where(s == me, jnp.logical_not(mine), lax.rem(s, m) != lat)
        else:
            due = (s != me) | jnp.logical_not(mine)

        @pl.when(due)
        def _():
            arrival(slot, s).wait_recv()

    def heads_of(slot):
        return share if slot == shared else HEADS

    def project_queries(slot):
        span = heads_of(slot) * head_width
        for b in range(blocks):
            cell_rows = x[slot, pl.ds(group * chips + b * pair, pair)].reshape(block, width)
            q_t = (dot(weight(0, slot), cell_rows, (1, 1)) * (1.0 / math.sqrt(head_width))).astype(jnp.bfloat16)
            q_t = q_t.astype(jnp.float32) * LOG2E
            q_hi = q_t.astype(jnp.bfloat16)
            q_lo = (q_t - q_hi.astype(jnp.float32)).astype(jnp.bfloat16)
            q_s[slot, 0:span, b * block:(b + 1) * block] = q_hi
            q_s[slot, width:width + span, b * block:(b + 1) * block] = q_lo

    def units(slot):
        return [0] if slot == shared else list(range(m))

    def prepare(slot, b, s0):
        cell_rows = x[slot, pl.ds(s0, pair)].reshape(block, width)
        for u in units(slot):
            kk_s[slot, u, b * block:(b + 1) * block, :] = dot(
                cell_rows, twice_s[int(slot == shared), u], (1, 1)).astype(jnp.bfloat16)
        v_s[slot, 0:heads_of(slot) * head_width, b * block:(b + 1) * block] = dot(
            weight(2, slot), cell_rows, (1, 1)).astype(jnp.bfloat16)

    def gap(size):
        return [jnp.zeros((size, queries), jnp.bfloat16)] if size else []

    def attend(items):
        def scores(slot, h, first, size):
            u, at = h // share, h % share * head_width
            lo, hi = h * head_width, (h + 1) * head_width
            before, after = gap(at), gap(half - head_width - at)
            spread_q = jnp.concatenate(
                before + [q_s[slot, lo:hi, :]] + after + before + [q_s[slot, width + lo:width + hi, :]] + after, axis=0)
            return dot(kk_s[slot, u, first:first + size, :], spread_q, (1, 0))

        def keep(i, s, c, part):
            piece = s[c * step:(c + 1) * step]
            scores_s[i % 2, c * step:(c + 1) * step, :] = piece
            part_max = jnp.max(piece.reshape(step // 8, 8, queries), axis=0)
            return part_max if part is None else jnp.maximum(part, part_max)

        def weigh(i, fade):
            slot, h, first, size = items[i]
            at = slot * HEADS + h
            acc_s[at] = acc_s[at] * fade + dot(
                v_s[slot, h * head_width:(h + 1) * head_width, first:first + size], p_s[i % 2, 0:size], (1, 0))

        s, part = scores(*items[0]), None
        for c in range(items[0][3] // step):
            part = keep(0, s, c, part)
        fade = None
        for i, (slot, h, first, size) in enumerate(items):
            highest = jnp.max(part, axis=0, keepdims=True)
            s = scores(*items[i + 1]) if i + 1 < len(items) else None
            if i:
                weigh(i - 1, fade)
            at = slot * HEADS + h
            before = top_s[at]
            now = jnp.maximum(before, highest)
            fade = jnp.exp2(before - now)
            top_s[at] = now
            part = total = None
            for c in range(size // step):
                p = jnp.exp2(scores_s[i % 2, c * step:(c + 1) * step, :] - now)
                piece = jnp.sum(p.reshape(step // 8, 8, queries), axis=0)
                total = piece if total is None else total + piece
                p_s[i % 2, c * step:(c + 1) * step, :] = p.astype(jnp.bfloat16)
                if s is not None:
                    part = keep(i + 1, s, c, part)
            sum_s[at] = sum_s[at] * fade + total
        weigh(len(items) - 1, fade)

    def await_group(slot, k):
        for c in range(chips):
            await_source(slot, lax.rem(group + k, groups) * chips + c)

    def prepare_group(slot, k):
        for b in range(blocks):
            prepare(slot, b, lax.rem(group + k, groups) * chips + b * pair)

    def unit_items(slot, u):
        wide = min(TILE, queries)
        return [(slot, u * share + h, first, wide) for first in range(0, queries, wide) for h in range(share)]

    def back(slot, u, c):
        hf = lat if slot == shared else u
        row = slot_row(slot)
        lon = group * chips + c
        copy = remote(mixed.at[slot, u, c], returned.at[row, hf], send2.at[slot, u, c], recv2.at[row, hf],
                      lon, source_lat)
        return row, hf, (lon != me) | (source_lat != lat), copy

    def hand_back(slot, u):
        for j in range(share):
            at = slot * HEADS + u * share + j
            done = (acc_s[at] / jnp.sum(sum_s[at], axis=0, keepdims=True)).astype(jnp.bfloat16)
            for c in range(chips):
                mixed[slot, u, c, j * head_width:(j + 1) * head_width, :] = done[:, c * cells:(c + 1) * cells]
        for c in range(chips):
            row, hf, away, copy = back(slot, u, c)

            @pl.when(away)
            def _():
                copy.start()

            @pl.when(jnp.logical_not(away))
            def _():
                returned[row, hf] = mixed[slot, u, c]

    pass_on(0)
    for slot in slots:
        await_group(slot, 0)
        project_queries(slot)
        prepare_group(slot, 0)
        attend([item for u in units(slot) for item in unit_items(slot, u)])
    for k in range(1, groups):
        pass_on(k)
        for slot in slots[::-1]:
            await_group(slot, k)
            prepare_group(slot, k)
            for u in units(slot):
                attend(unit_items(slot, u))
                if k == groups - 1:
                    hand_back(slot, u)

    each_forward(lambda copy: copy.wait_send(), range(groups))
    if shared is not None:
        for s in range(n):
            @pl.when((s != me) & (s % m == lat))
            def _():
                relay(s).wait_send()
    for slot in slots:
        for u in units(slot):
            for c in range(chips):
                row, hf, away, copy = back(slot, u, c)

                @pl.when(away)
                def _():
                    copy.wait_send()

    for r in range(rows):
        w = r % rpc
        lon = group * chips + lat * per_lat + r // rpc
        for hf in range(m):
            core = 0 if w < full else 1 if w >= rpc - full else hf

            @pl.when((lon != me) | (core != lat))
            def _():
                remote(mixed.at[0, 0, 0], returned.at[r, hf], send2.at[0, 0, 0], recv2.at[r, hf], lon, core).wait_recv()
        att_t = returned[r].reshape(width, cells)
        update = dot(att_t, wout_ref[...], (0, 0))
        out_ref[r] = (fields_ref[r].astype(jnp.float32) + update).astype(jnp.bfloat16)


def solution(mesh):
    n, m = mesh.shape["lon"], mesh.shape["lat"]

    def body(fields, norm_gain, w_qkv, w_out):
        rows, cells, width = fields.shape
        chips, rpc, full = plan(n, m, rows)
        groups, slots = n // chips, full + (1 if rpc % m else 0)
        queries, block = chips * cells, 2 * cells
        head_width = width // HEADS
        half = width // m
        bf16, f32 = jnp.bfloat16, jnp.float32
        return pl.pallas_call(
            functools.partial(kernel, n, m),
            out_shape=pltpu.VMEM(fields.shape, fields.dtype),
            in_specs=[pl.BlockSpec(memory_space=pltpu.HBM)] * 4,
            out_specs=pl.BlockSpec(memory_space=pltpu.VMEM),
            scratch_shapes=[
                pltpu.VMEM(fields.shape, fields.dtype),
                pltpu.VMEM((1, width), norm_gain.dtype),
                pltpu.VMEM(w_qkv.shape, w_qkv.dtype),
                pltpu.VMEM(w_out.shape, w_out.dtype),
                pltpu.VMEM((rows, cells, width), bf16),
                pltpu.VMEM((3 * width, width), bf16),
                pltpu.VMEM((2, m, 2 * half, width), bf16),
                pltpu.VMEM((slots, n, cells, width), bf16),
                pltpu.VMEM((2, min(TILE, queries), queries), f32),
                pltpu.VMEM((2, min(TILE, queries), queries), bf16),
                pltpu.VMEM((slots, 2 * width, queries), bf16),
                pltpu.VMEM((slots, m, queries, 2 * half), bf16),
                pltpu.VMEM((slots, width, queries), bf16),
                pltpu.VMEM((slots * HEADS, 1, queries), f32),
                pltpu.VMEM((slots * HEADS, 8, queries), f32),
                pltpu.VMEM((slots * HEADS, head_width, queries), f32),
                pltpu.VMEM((slots, m, chips, half, cells), bf16),
                pltpu.VMEM((rows, m, half, cells), bf16),
                pltpu.SemaphoreType.DMA((4,)),
                pltpu.SemaphoreType.DMA((groups, rows)),
                pltpu.SemaphoreType.DMA((rows,)),
                pltpu.SemaphoreType.DMA((slots, n)),
                pltpu.SemaphoreType.DMA((n,)),
                pltpu.SemaphoreType.DMA((slots, m, chips)),
                pltpu.SemaphoreType.DMA((rows, m)),
                pltpu.SemaphoreType.REGULAR,
                pltpu.SemaphoreType.REGULAR,
                pltpu.SemaphoreType.REGULAR,
            ],
            compiler_params=pltpu.CompilerParams(
                collective_id=0, has_side_effects=True, vmem_limit_bytes=40 * 2**20,
            ),
        )(*(
            pltpu.with_memory_space_constraint(x, pltpu.HBM)
            for x in (fields, norm_gain.reshape(1, width), w_qkv, w_out)
        ))

    return jax.shard_map(
        body,
        mesh=mesh,
        in_specs=(P(("groups", "lat"), "lon", None), P(), P(), P()),
        out_specs=P(("groups", "lat"), "lon", None),
        check_vma=False,
    )
```
